32 devices in a mesh: groups: 2 (over y), ep: 16 (over z, x, core).
Axes of the slice: x: 2, y: 2, z: 4, core: 2. Of those that a mesh axis runs over, the one named last changes fastest.
Arguments:
- tokens: bfloat16 [512, 2880], P(('groups', 'ep')), parts along dimension 0, may hold values from -6 to 6
- routes: int32 [512, 4], P(('groups', 'ep')), parts along dimension 0, may hold values from 0 to 7, all different within a row; in each aligned block of 16 rows (0 to 15, 16 to 31, ...) at most 16 rows name the same one
- gate_fixed: int32 [512, 4], P(('groups', 'ep')), parts along dimension 0, may hold values from 1 to 65535
- gate_weight: bfloat16 [16, 2880, 720], P('ep'), may hold values from -0.109375 to 0.109375
- up_weight: bfloat16 [16, 2880, 720], P('ep'), may hold values from -0.109375 to 0.109375
- down_weight: bfloat16 [16, 720, 2880], P('ep'), may hold values from -0.15625 to 0.15625
Outputs:
- mixed: bfloat16 [512, 2880], P(('groups', 'ep')), parts along dimension 0
The draws below stay inside these ranges and needn't reach their ends.
There are 2 independent parts, one for each index of `groups`. The reference program is written for one: setup_inputs(seed, part) draws one part's arguments, and reference() takes and returns one part's arrays. A program takes and returns all parts, laid end to end along the dimension named above; an argument that names none is the same for every part. Nothing has to cross between parts.
Inputs may be any that keep to these rules, and one draw needn't show every extreme that they name: `routes`: each row names 4 different experts; the 16 rows of one device name any one expert at most 16 times.
All inputs are finite; a program needn't handle non-finite values.
Results may differ from the reference program's by a relative error of at most 0.0065.
Values may be sent and summed in bfloat16 or wider, within the bound.
A program may use at most 64 MiB of HBM per device.

```python
import math
import jax
import jax.numpy as jnp
import numpy as np
from jax import lax

D = 2880
FF = 1440
TOP = 4
TOK_DEV = 16
HALF = 720
EXPERTS = 8
TOKENS = 256
CAP = 16
N_EP = 16


def set_ends(values, stream_key, least, high):
    longest = values.shape.index(max(values.shape))
    spots = []
    for shift in (0, 1):
        where = [jax.random.randint(jax.random.fold_in(stream_key, axis), (), 0, length) for axis, length in enumerate(values.shape)]
        where[longest] = (where[longest] + shift) % values.shape[longest]
        spots.append(tuple(where))
    return values.at[spots[0]].set(least).at[spots[1]].set(high)


def block_levels(rng, extent, split, least, top_value):
    level, own = 1.0, jax.random.fold_in(rng, 6)
    for dim, parts in split:
        steps = jnp.exp(jax.random.uniform(jax.random.fold_in(own, dim), (parts,), jnp.float32, least / len(split), top_value / len(split)))
        level = level * jnp.repeat(steps, extent[dim] // parts).reshape([-1 if axis == dim else 1 for axis in range(len(extent))])
    return level


def shared_out(stream_key, own, number, rows, amount, top, reach, lean):
    sequence = jax.random.permutation(stream_key, amount)
    heavy_load, ordinary = shares(amount, rows * top, reach, lean, True), shares(amount, rows * top, reach, lean, False)
    places = jnp.arange(amount)

    def named(lengths, turn):
        used = int((lengths > 0).sum())
        fixed = max(1, used // 4)
        moved = fixed + (places - fixed + turn * (used - fixed)) % max(1, amount - fixed)
        return jnp.zeros((amount,), jnp.int32).at[sequence[jnp.where(places < fixed, places, moved)]].set(jnp.asarray(lengths, jnp.int32))

    lengths = jnp.where(number % 4 == 0, named(heavy_load, number // 4), named(ordinary, number - number // 4 - 1))
    mixed = jax.random.permutation(jax.random.fold_in(own, 3), amount)
    giver, receiver = mixed[0:amount // 2 * 2:2], mixed[1:amount // 2 * 2:2]
    margin = jnp.minimum(lengths[giver] - 1, reach - lengths[receiver]) // 2
    margin = jnp.where((giver == sequence[0]) | (receiver == sequence[0]) | (lengths[receiver] == 0), 0, jnp.maximum(margin, 0))
    moved = jax.random.randint(jax.random.fold_in(own, 4), (amount // 2,), 0, 1 << 20) % (margin + 1)
    lengths = lengths.at[giver].add(-moved).at[receiver].add(moved)
    members = jnp.searchsorted(jnp.cumsum(lengths), jnp.arange(rows * top), side="right").astype(jnp.int32)
    grid = members.reshape(top, rows).T
    grid = grid[jax.random.permutation(jax.random.fold_in(own, 1), rows)]
    turn = jax.random.randint(jax.random.fold_in(own, 2), (rows, 1), 0, top)
    return jnp.take_along_axis(grid, (jnp.arange(top)[None, :] + turn) % top, axis=1)


def shares(count, total, limit, lean, full):
    weights = [(1 << 20) // math.isqrt(standing ** lean) + 1 for standing in range(1, count + 1)]
    largest = limit if full else min(limit, max(-(-total // count), total * weights[0] // sum(weights)))
    least = 1 if total - largest >= count - 1 else 0
    given, surplus = [largest] + [least] * (count - 1), total - largest - least * (count - 1)
    while surplus > 0:
        free = [i for i in range(1, count) if given[i] < largest] or [i for i in range(1, count) if given[i] < limit]
        pool, budget = sum([weights[i] for i in free]), surplus
        for i in free:
            more = min(limit - given[i], max(1, budget * weights[i] // pool), surplus)
            given[i] = given[i] + more
            surplus = surplus - more
    return np.array(given)


def noise(own_key, dims, spread, limit, shards=(), kind=jnp.bfloat16):
    drawn = jax.random.normal(own_key, dims, jnp.float32) * spread
    if len(shards) > 0:
        drawn = block_levels(own_key, dims, shards, -0.22, 0.18) * drawn
    return jnp.clip(drawn, min=-limit, max=limit).astype(kind)


def setup_inputs(seed: int = 0, part: int = 0) -> dict:
    streams_of = jax.random.split(jax.random.key(seed), 7)
    part_keys = jax.random.split(jax.random.fold_in(streams_of[6], part), 7)
    tokens = noise(part_keys[0], (TOKENS, D), 1.0, 6.0, ((0, 16),))
    routes_keys = jax.random.split(jax.random.fold_in(part_keys[1], 1), TOKENS // TOK_DEV)
    routes_turns = jax.random.permutation(jax.random.fold_in(part_keys[1], 3), TOKENS // TOK_DEV)
    routes = jax.vmap(lambda own, number: shared_out(jax.random.fold_in(part_keys[1], 2), own, number, TOK_DEV, EXPERTS, TOP, CAP, 2))(routes_keys, routes_turns).reshape((TOKENS, TOP))
    gate_fixed = set_ends(jax.random.randint(part_keys[2], (TOKENS, TOP), 1, 65536), jax.random.fold_in(part_keys[2], 1), 1, 65535).astype(jnp.int32)
    gate_weight = noise(streams_of[3], (N_EP, D, HALF), D ** -0.5, 0.109375, ((0, 16),))
    up_weight = noise(streams_of[4], (N_EP, D, HALF), D ** -0.5, 0.109375, ((0, 16),))
    down_weight = noise(streams_of[5], (N_EP, HALF, D), FF ** -0.5, 0.15625, ((0, 16),))
    return dict(tokens=tokens, routes=routes, gate_fixed=gate_fixed, gate_weight=gate_weight, up_weight=up_weight, down_weight=down_weight)


def reference(tokens, routes, gate_fixed, gate_weight, up_weight, down_weight):
    experts = N_EP // 2
    onehot = (routes[:, :, None] == jnp.arange(experts, dtype=jnp.int32)).astype(jnp.int32)
    grouped = onehot.reshape(N_EP, TOK_DEV * TOP, experts)
    before = jnp.cumsum(grouped, axis=1) - grouped
    position = jnp.sum(before * grouped, axis=-1).reshape(TOKENS, TOP).astype(jnp.int32)
    source = (jnp.arange(TOKENS, dtype=jnp.int32) // TOK_DEV)[:, None]
    column = (source * CAP + position).astype(jnp.int32)
    token_ids = jnp.broadcast_to(jnp.arange(TOKENS, dtype=jnp.int32)[:, None], (TOKENS, TOP))
    slot_table = jnp.full((experts, N_EP * CAP), TOKENS, jnp.int32).at[routes, column].set(token_ids)
    padded = jnp.concatenate([tokens, jnp.zeros((1, D), tokens.dtype)], axis=0)

    def half_part(expert_rows, index):
        w_gate = lax.dynamic_index_in_dim(gate_weight, index, 0, keepdims=False)
        w_up = lax.dynamic_index_in_dim(up_weight, index, 0, keepdims=False)
        w_down = lax.dynamic_index_in_dim(down_weight, index, 0, keepdims=False)
        gate_part = jnp.dot(expert_rows, w_gate, preferred_element_type=jnp.float32)
        up_part = jnp.dot(expert_rows, w_up, preferred_element_type=jnp.float32)
        hidden = (jax.nn.silu(gate_part) * up_part).astype(jnp.bfloat16)
        return jnp.dot(hidden, w_down, preferred_element_type=jnp.float32).astype(jnp.bfloat16)

    def run_expert(expert):
        expert_rows = padded[slot_table[expert]]
        first = (2 * expert).astype(jnp.int32)
        lower = half_part(expert_rows, first)
        upper = half_part(expert_rows, (first + 1).astype(jnp.int32))
        return (lower.astype(jnp.float32) + upper.astype(jnp.float32)).astype(jnp.bfloat16)

    outputs = lax.map(run_expert, jnp.arange(experts, dtype=jnp.int32))
    picked = outputs[routes, column]
    weights = gate_fixed.astype(jnp.float32) / 65536.0
    mixed = jnp.sum(weights[:, :, None] * picked.astype(jnp.float32), axis=1)
    return mixed.astype(jnp.bfloat16)
```

```python
import functools

import jax
import jax.numpy as jnp
from jax import lax
from jax.experimental import pallas as pl
from jax.experimental.pallas import tpu as pltpu
from jax.sharding import PartitionSpec as P


def swapped(value, axis, bit):
    mask = 2**bit
    pairs = [(source, source ^ mask) for source in range(lax.axis_size(axis))]
    return lax.ppermute(value, axis, pairs)


def expert_half(expert_rows, w_gate, w_up, w_down):
    gate_part = jnp.dot(expert_rows, w_gate, preferred_element_type=jnp.float32)
    up_part = jnp.dot(expert_rows, w_up, preferred_element_type=jnp.float32)
    hidden = (jax.nn.silu(gate_part) * up_part).astype(jnp.bfloat16)
    return jnp.dot(hidden, w_down, preferred_element_type=jnp.float32).astype(jnp.bfloat16)


def local(tokens, routes, gate_fixed, gate_weight, up_weight, down_weight):
    devices_ep = lax.axis_size("ep")
    experts = devices_ep // 2
    tok_count = tokens.shape[0]
    top_count = routes.shape[1]
    width = tokens.shape[1]
    capacity = 2 * tok_count * top_count // experts
    onehot = (routes[:, :, None] == jnp.arange(experts, dtype=jnp.int32)).astype(jnp.int32)
    flat_hot = onehot.reshape(tok_count * top_count, experts)
    before = jnp.cumsum(flat_hot, axis=0) - flat_hot
    position = jnp.sum(before * flat_hot, axis=1).reshape(tok_count, top_count)
    slot_index = routes * capacity + position
    select = (slot_index[:, :, None] == jnp.arange(experts * capacity, dtype=jnp.int32)).astype(
        jnp.int32
    )
    select = jnp.sum(select, axis=1).astype(jnp.bfloat16)
    packed = jnp.einsum("ts,td->sd", select, tokens, preferred_element_type=jnp.float32).astype(
        jnp.bfloat16
    )
    packed = packed.reshape(experts, 1, capacity, width)
    outgoing = jnp.broadcast_to(packed, (experts, 2, capacity, width)).reshape(
        devices_ep, capacity, width
    )
    received = lax.all_to_all(outgoing, "ep", split_axis=0, concat_axis=0, tiled=True)
    result = expert_half(received.reshape(-1, width), gate_weight[0], up_weight[0], down_weight[0])
    partial_value = result.reshape(received.shape[0], received.shape[1], width)
    parity = lax.axis_index("ep") % 2
    halves = partial_value.reshape(devices_ep, capacity, 2, width // 2)
    kept_half = lax.dynamic_index_in_dim(halves, parity, 2, keepdims=False)
    given_half = lax.dynamic_index_in_dim(halves, 1 - parity, 2, keepdims=False)
    partner = swapped(given_half, "ep", 0)
    reduced = (kept_half.astype(jnp.float32) + partner.astype(jnp.float32)).astype(jnp.bfloat16)
    returned = lax.all_to_all(reduced, "ep", split_axis=0, concat_axis=0, tiled=True)
    ordered = returned.reshape(experts, 2, capacity, width // 2).transpose(0, 2, 1, 3)
    expert_out = ordered.reshape(experts * capacity, width)
    picked = jnp.take(expert_out, slot_index.reshape(-1), axis=0).reshape(
        tok_count, top_count, width
    )
    weights = gate_fixed.astype(jnp.float32) / 65536.0
    mixed = jnp.sum(weights[:, :, None] * picked.astype(jnp.float32), axis=1)
    return mixed.astype(jnp.bfloat16)


def ordered_offsets(count):
    return sorted(range(1, count), key=lambda off: (-min(off, count - off), off)) + [0]


def column_cuts(width, step):
    return [(low, min(low + step, width)) for low in range(0, width, step)]


def dense_kernel(
    slow, fast, tokens, routes, gates, w_gate, w_up, w_down, out,
    gathered, vm_gate, vm_up, vm_down, partial, from_core, to_fast, from_fast, to_slow, from_slow,
    w_sem, ag_send, ag_recv, core_send, core_recv, fast_send, fast_recv, slow_send, slow_recv,
    pass_send, pass_recv, give_send, give_recv,
):
    rows, width = tokens.shape
    top = routes.shape[1]
    padded = gathered.shape[1]
    hidden_count = vm_gate.shape[1]
    offsets = ordered_offsets(slow)
    device = lax.axis_index("ep")
    core = lax.rem(device, 2)
    chip = device // 2
    at_slow = chip // fast
    at_fast = lax.rem(chip, fast)

    weights = [
        pltpu.make_async_copy(source.at[0], target, w_sem.at[i])
        for i, (source, target) in enumerate(((w_gate, vm_gate), (w_up, vm_up), (w_down, vm_down)))
    ]
    for copy in weights:
        copy.start()

    def name(s, f, c):
        return {"ep": (s * fast + f) * 2 + c}

    def slow_at(off):
        return lax.rem(at_slow + off, slow)

    def fast_at(off):
        return lax.rem(at_fast + off, fast)

    def block(s, f, c):
        start = ((s * 2 + c) * fast + f) * rows
        return pl.ds(pl.multiple_of(start, rows), rows)

    def send(source, target, send_sem, recv_sem, device_id):
        return pltpu.make_async_remote_copy(
            src_ref=source, dst_ref=target, send_sem=send_sem, recv_sem=recv_sem,
            device_id=device_id, device_id_type=pl.DeviceIdType.MESH,
        )

    peers = [name(slow_at(off), at_fast, core) for off in range(1, slow)]
    peers += [name(at_slow, fast_at(off), core) for off in range(1, fast)]
    peers += [name(at_slow, at_fast, 1 - core)]
    barrier = pltpu.get_barrier_semaphore()
    for peer in peers:
        pl.semaphore_signal(barrier, inc=1, device_id=peer, device_id_type=pl.DeviceIdType.MESH)

    mine = block(at_slow, at_fast, core)
    edge = width // 128 * 128
    lanes = lax.broadcasted_iota(jnp.int32, (rows, padded - edge), 1) + edge
    gathered[mine, edge:] = jnp.zeros((rows, padded - edge), jnp.bfloat16)
    gathered[mine, :width] = tokens[...]
    scale = gates[...].astype(jnp.float32) / 65536.0
    high = scale.astype(jnp.bfloat16).astype(jnp.float32)
    low = scale - high
    ids = routes[...].astype(jnp.float32)
    tail = gathered[mine, edge:].astype(jnp.float32)
    for k in range(top):
        tail = jnp.where(lanes == width + k, ids[:, k : k + 1], tail)
        tail = jnp.where(lanes == width + top + k, high[:, k : k + 1], tail)
        tail = jnp.where(lanes == width + 2 * top + k, low[:, k : k + 1], tail)
    gathered[mine, edge:] = tail.astype(jnp.bfloat16)

    pl.semaphore_wait(barrier, len(peers))

    started = []

    def launch(copy):
        copy.start()
        started.append(copy)

    def to_partner(s, f, slot):
        where = gathered.at[block(s, f, core)]
        launch(send(where, where, core_send.at[slot], core_recv.at[slot], name(at_slow, at_fast, 1 - core)))

    def along_fast(s, step):
        where = gathered.at[block(s, at_fast, core)]
        for off in range(1, fast):
            launch(send(where, where, fast_send.at[step, off], fast_recv.at[step, off], name(at_slow, fast_at(off), core)))

    here = gathered.at[mine]
    along_fast(at_slow, slow - 1)
    for step, off in enumerate(offsets[:-1]):
        launch(send(here, here, ag_send.at[step], ag_recv.at[step], name(slow_at(off), at_fast, core)))
    to_partner(at_slow, at_fast, 0)

    slot = 1
    for step, off in enumerate(offsets):
        if off:
            s = slow_at(slow - off)
            got = gathered.at[block(s, at_fast, core)]
            send(got, got, ag_send.at[step], ag_recv.at[step], name(s, at_fast, core)).wait_recv()
            along_fast(s, step)
            to_partner(s, at_fast, slot)
            slot += 1
    for step in [slow - 1] + list(range(slow - 1)):
        s = slow_at(slow - offsets[step])
        for off in range(1, fast):
            f = fast_at(fast - off)
            got = gathered.at[block(s, f, core)]
            send(got, got, fast_send.at[step, off], fast_recv.at[step, off], name(at_slow, f, core)).wait_recv()
            to_partner(s, f, slot)
            slot += 1
    slot = 0
    arrivals = [(at_slow, at_fast)] + [(slow_at(slow - off), at_fast) for off in offsets[:-1]]
    for step in [slow - 1] + list(range(slow - 1)):
        arrivals += [(slow_at(slow - offsets[step]), fast_at(fast - off)) for off in range(1, fast)]
    for slot, (s, f) in enumerate(arrivals):
        got = gathered.at[block(s, f, 1 - core)]
        send(got, got, core_send.at[slot], core_recv.at[slot], name(at_slow, at_fast, 1 - core)).wait_recv()

    weights[0].wait()
    weights[1].wait()
    expert = chip.astype(jnp.float32)
    info = gathered[:, edge:].astype(jnp.float32)
    factor = jnp.zeros((info.shape[0], 1), jnp.float32)
    for k in range(top):
        col = width - edge + k
        value = info[:, col + top : col + top + 1] + info[:, col + 2 * top : col + 2 * top + 1]
        factor += jnp.where(info[:, col : col + 1] == expert, value, 0.0)
    x = gathered[:, :width]
    pieces = []
    for low_col, high_col in column_cuts(hidden_count, 256):
        g = jnp.dot(x, vm_gate[:, low_col:high_col], preferred_element_type=jnp.float32)
        u = jnp.dot(x, vm_up[:, low_col:high_col], preferred_element_type=jnp.float32)
        pieces.append((jax.nn.silu(g) * u).astype(jnp.bfloat16))
    hidden = jnp.concatenate(pieces, axis=1)
    weights[2].wait()
    for low_col, high_col in column_cuts(width, 512):
        y = jnp.dot(hidden, vm_down[:, low_col:high_col], preferred_element_type=jnp.float32)
        partial[:, low_col:high_col] = (y * factor).astype(jnp.bfloat16)

    def pair(s, c):
        return pl.ds(pl.multiple_of((s * 2 + c) * fast * rows, rows), fast * rows)

    def tile(index):
        return pl.ds(pl.multiple_of(index * rows, rows), rows)

    def core_copy(step):
        s = slow_at(offsets[step])
        return send(
            partial.at[pair(s, 1 - core)], from_core.at[pl.ds(step * fast * rows, fast * rows)],
            pass_send.at[step], pass_recv.at[step], name(at_slow, at_fast, 1 - core),
        )

    def both_cores(step, f):
        s = slow_at(offsets[step])
        mine_part = partial[block(s, f, core), :].astype(jnp.float32)
        return mine_part + from_core[tile(step * fast + f), :].astype(jnp.float32)

    def fast_copy(step, off):
        place = pl.ds((step * (fast - 1) + off - 1) * rows, rows)
        return send(
            to_fast.at[place], from_fast.at[place],
            give_send.at[step, off], give_recv.at[step, off], name(at_slow, fast_at(off), core),
        )

    def slow_copy(step):
        place = pl.ds(step * rows, rows)
        return send(
            to_slow.at[place], from_slow.at[place],
            slow_send.at[step], slow_recv.at[step], name(slow_at(offsets[step]), at_fast, core),
        )

    for step in range(slow):
        launch(core_copy(step))
    for step in range(slow):
        core_copy(step).wait_recv()
        for off in range(1, fast):
            place = (step * (fast - 1) + off - 1) * rows
            to_fast[place : place + rows, :] = both_cores(step, fast_at(off)).astype(jnp.bfloat16)
            launch(fast_copy(step, off))
    for step in range(slow):
        total = both_cores(step, at_fast)
        for off in range(1, fast):
            fast_copy(step, off).wait_recv()
            place = (step * (fast - 1) + off - 1) * rows
            total += from_fast[place : place + rows, :].astype(jnp.float32)
        if offsets[step]:
            to_slow[step * rows : (step + 1) * rows, :] = total.astype(jnp.bfloat16)
            launch(slow_copy(step))
    for step in range(slow - 1):
        slow_copy(step).wait_recv()
        total += from_slow[step * rows : (step + 1) * rows, :].astype(jnp.float32)
    out[...] = total.astype(out.dtype)
    for copy in started:
        copy.wait_send()


def dense_local(slow, fast, tokens, routes, gate_fixed, gate_weight, up_weight, down_weight):
    rows, width = tokens.shape
    top = routes.shape[1]
    hidden_count = gate_weight.shape[2]
    padded = -(-(width + 3 * top) // 128) * 128
    every = slow * fast * 2 * rows
    dma = pltpu.SemaphoreType.DMA
    half = slow * fast * rows
    vmem = pl.BlockSpec(memory_space=pltpu.VMEM)
    anywhere = pl.BlockSpec(memory_space=pl.ANY)
    return pl.pallas_call(
        functools.partial(dense_kernel, slow, fast),
        out_shape=jax.ShapeDtypeStruct((rows, width), jnp.bfloat16),
        in_specs=[vmem, vmem, vmem, anywhere, anywhere, anywhere],
        out_specs=vmem,
        scratch_shapes=[
            pltpu.VMEM((every, padded), jnp.bfloat16),
            pltpu.VMEM(gate_weight.shape[1:], jnp.bfloat16),
            pltpu.VMEM(up_weight.shape[1:], jnp.bfloat16),
            pltpu.VMEM(down_weight.shape[1:], jnp.bfloat16),
            pltpu.VMEM((every, width), jnp.bfloat16),
            pltpu.VMEM((half, width), jnp.bfloat16),
            pltpu.VMEM((slow * (fast - 1) * rows, width), jnp.bfloat16),
            pltpu.VMEM((slow * (fast - 1) * rows, width), jnp.bfloat16),
            pltpu.VMEM(((slow - 1) * rows, width), jnp.bfloat16),
            pltpu.VMEM(((slow - 1) * rows, width), jnp.bfloat16),
            dma((3,)),
            dma((slow,)), dma((slow,)),
            dma((slow * fast,)), dma((slow * fast,)),
            dma((slow, fast)), dma((slow, fast)),
            dma((slow,)), dma((slow,)),
            dma((slow,)), dma((slow,)),
            dma((slow, fast)), dma((slow, fast)),
        ],
        compiler_params=pltpu.CompilerParams(
            collective_id=0, has_side_effects=True, vmem_limit_bytes=60 * 2**20
        ),
    )(tokens, routes, gate_fixed, gate_weight, up_weight, down_weight)


def solution(mesh):
    placed = (
        P(("groups", "ep"), None),
        P(("groups", "ep"), None),
        P(("groups", "ep"), None),
        P("ep", None, None),
        P("ep", None, None),
        P("ep", None, None),
    )
    chips = mesh.shape["ep"] // 2

    def body(*args):
        top = args[1].shape[1]
        if chips <= 4 * top and chips % 4 == 0:
            return dense_local(4, chips // 4, *args)
        return local(*args)

    return jax.shard_map(
        body, mesh=mesh, in_specs=placed, out_specs=P(("groups", "ep"), None), check_vma=False
    )
```

```python
import functools

import jax
import jax.numpy as jnp
from jax import lax
from jax.experimental import pallas as pl
from jax.experimental.pallas import tpu as pltpu
from jax.sharding import PartitionSpec as P


def swapped(value, axis, bit):
    mask = 2**bit
    pairs = [(source, source ^ mask) for source in range(lax.axis_size(axis))]
    return lax.ppermute(value, axis, pairs)


def expert_half(expert_rows, w_gate, w_up, w_down):
    gate_part = jnp.dot(expert_rows, w_gate, preferred_element_type=jnp.float32)
    up_part = jnp.dot(expert_rows, w_up, preferred_element_type=jnp.float32)
    hidden = (jax.nn.silu(gate_part) * up_part).astype(jnp.bfloat16)
    return jnp.dot(hidden, w_down, preferred_element_type=jnp.float32).astype(jnp.bfloat16)


def local(tokens, routes, gate_fixed, gate_weight, up_weight, down_weight):
    devices_ep = lax.axis_size("ep")
    experts = devices_ep // 2
    tok_count = tokens.shape[0]
    top_count = routes.shape[1]
    width = tokens.shape[1]
    capacity = 2 * tok_count * top_count // experts
    onehot = (routes[:, :, None] == jnp.arange(experts, dtype=jnp.int32)).astype(jnp.int32)
    flat_hot = onehot.reshape(tok_count * top_count, experts)
    before = jnp.cumsum(flat_hot, axis=0) - flat_hot
    position = jnp.sum(before * flat_hot, axis=1).reshape(tok_count, top_count)
    slot_index = routes * capacity + position
    select = (slot_index[:, :, None] == jnp.arange(experts * capacity, dtype=jnp.int32)).astype(
        jnp.int32
    )
    select = jnp.sum(select, axis=1).astype(jnp.bfloat16)
    packed = jnp.einsum("ts,td->sd", select, tokens, preferred_element_type=jnp.float32).astype(
        jnp.bfloat16
    )
    packed = packed.reshape(experts, 1, capacity, width)
    outgoing = jnp.broadcast_to(packed, (experts, 2, capacity, width)).reshape(
        devices_ep, capacity, width
    )
    received = lax.all_to_all(outgoing, "ep", split_axis=0, concat_axis=0, tiled=True)
    result = expert_half(received.reshape(-1, width), gate_weight[0], up_weight[0], down_weight[0])
    partial_value = result.reshape(received.shape[0], received.shape[1], width)
    parity = lax.axis_index("ep") % 2
    halves = partial_value.reshape(devices_ep, capacity, 2, width // 2)
    kept_half = lax.dynamic_index_in_dim(halves, parity, 2, keepdims=False)
    given_half = lax.dynamic_index_in_dim(halves, 1 - parity, 2, keepdims=False)
    partner = swapped(given_half, "ep", 0)
    reduced = (kept_half.astype(jnp.float32) + partner.astype(jnp.float32)).astype(jnp.bfloat16)
    returned = lax.all_to_all(reduced, "ep", split_axis=0, concat_axis=0, tiled=True)
    ordered = returned.reshape(experts, 2, capacity, width // 2).transpose(0, 2, 1, 3)
    expert_out = ordered.reshape(experts * capacity, width)
    picked = jnp.take(expert_out, slot_index.reshape(-1), axis=0).reshape(
        tok_count, top_count, width
    )
    weights = gate_fixed.astype(jnp.float32) / 65536.0
    mixed = jnp.sum(weights[:, :, None] * picked.astype(jnp.float32), axis=1)
    return mixed.astype(jnp.bfloat16)


NT = (((1,), (1,)), ((), ()))


def ordered_offsets(count):
    return sorted(range(1, count), key=lambda off: (-min(off, count - off), off)) + [0]


def column_cuts(width, step):
    return [(low, min(low + step, width)) for low in range(0, width, step)]


def dense_kernel(
    slow, fast, tokens, routes, gates, w_gate, w_up, w_down, out,
    gathered, vm_gate, vm_up, vm_down, partial, from_core, to_fast, from_fast, to_slow, from_slow,
    w_sem, ag_send, ag_recv, core_send, core_recv, fast_send, fast_recv, slow_send, slow_recv,
    pass_send, pass_recv, give_send, give_recv,
):
    rows, width = tokens.shape
    top = routes.shape[0]
    padded = gathered.shape[1]
    hidden_count = vm_gate.shape[0]
    offsets = ordered_offsets(slow)
    device = lax.axis_index("ep")
    core = lax.rem(device, 2)
    chip = device // 2
    at_slow = chip // fast
    at_fast = lax.rem(chip, fast)

    weights = [
        pltpu.make_async_copy(source.at[0], target, w_sem.at[i])
        for i, (source, target) in enumerate(((w_gate, vm_gate), (w_up, vm_up), (w_down, vm_down)))
    ]
    for copy in weights:
        copy.start()

    def name(s, f, c):
        return {"ep": (s * fast + f) * 2 + c}

    def slow_at(off):
        return lax.rem(at_slow + off, slow)

    def fast_at(off):
        return lax.rem(at_fast + off, fast)

    def block(s, f, c):
        start = ((s * 2 + c) * fast + f) * rows
        return pl.ds(pl.multiple_of(start, rows), rows)

    def send(source, target, send_sem, recv_sem, device_id):
        return pltpu.make_async_remote_copy(
            src_ref=source, dst_ref=target, send_sem=send_sem, recv_sem=recv_sem,
            device_id=device_id, device_id_type=pl.DeviceIdType.MESH,
        )

    peers = [name(slow_at(off), at_fast, core) for off in range(1, slow)]
    peers += [name(at_slow, fast_at(off), core) for off in range(1, fast)]
    peers += [name(at_slow, at_fast, 1 - core)]
    barrier = pltpu.get_barrier_semaphore()
    for peer in peers:
        pl.semaphore_signal(barrier, inc=1, device_id=peer, device_id_type=pl.DeviceIdType.MESH)

    mine = block(at_slow, at_fast, core)
    edge = width // 128 * 128
    lanes = lax.broadcasted_iota(jnp.int32, (rows, padded - edge), 1) + edge
    gathered[mine, edge:] = jnp.zeros((rows, padded - edge), jnp.bfloat16)
    gathered[mine, :width] = tokens[...]
    scale = jnp.transpose(gates[...].astype(jnp.float32)) / 65536.0
    high = scale.astype(jnp.bfloat16).astype(jnp.float32)
    low = scale - high
    ids = jnp.transpose(routes[...].astype(jnp.float32))
    tail = gathered[mine, edge:].astype(jnp.float32)
    for k in range(top):
        tail = jnp.where(lanes == width + k, ids[:, k : k + 1], tail)
        tail = jnp.where(lanes == width + top + k, high[:, k : k + 1], tail)
        tail = jnp.where(lanes == width + 2 * top + k, low[:, k : k + 1], tail)
    gathered[mine, edge:] = tail.astype(jnp.bfloat16)

    pl.semaphore_wait(barrier, len(peers))

    started = []

    def launch(copy):
        copy.start()
        started.append(copy)

    def to_partner(s, f, slot):
        where = gathered.at[block(s, f, core)]
        launch(send(where, where, core_send.at[slot], core_recv.at[slot], name(at_slow, at_fast, 1 - core)))

    def along_fast(s, step):
        where = gathered.at[block(s, at_fast, core)]
        for off in range(1, fast):
            launch(send(where, where, fast_send.at[step, off], fast_recv.at[step, off], name(at_slow, fast_at(off), core)))

    here = gathered.at[mine]
    along_fast(at_slow, slow - 1)
    for step, off in enumerate(offsets[:-1]):
        launch(send(here, here, ag_send.at[step], ag_recv.at[step], name(slow_at(off), at_fast, core)))
    to_partner(at_slow, at_fast, (slow - 1) * fast)

    own = slow - 1
    order = [own] + list(range(own))
    chunk_rows = 2 * fast * rows

    def source(step):
        return slow_at(slow - offsets[step])

    def take_slow(step):
        if step == own:
            return
        s = source(step)
        got = gathered.at[block(s, at_fast, core)]
        send(got, got, ag_send.at[step], ag_recv.at[step], name(s, at_fast, core)).wait_recv()
        along_fast(s, step)
        to_partner(s, at_fast, step * fast)

    def take_fast(step):
        for off in range(1, fast):
            f = fast_at(fast - off)
            got = gathered.at[block(source(step), f, core)]
            send(got, got, fast_send.at[step, off], fast_recv.at[step, off], name(at_slow, f, core)).wait_recv()
            to_partner(source(step), f, step * fast + off)

    def take_core(step):
        for off in range(fast):
            slot = step * fast + off
            got = gathered.at[block(source(step), fast_at(fast - off), 1 - core)]
            send(got, got, core_send.at[slot], core_recv.at[slot], name(at_slow, at_fast, 1 - core)).wait_recv()

    def chunk(step):
        return pl.ds(pl.multiple_of(source(step) * chunk_rows, chunk_rows), chunk_rows)

    def half_expert(steps):
        expert = chip.astype(jnp.float32)
        factors = []
        for step in steps:
            info = gathered[chunk(step), edge:].astype(jnp.float32)
            factor = jnp.zeros((chunk_rows, 1), jnp.float32)
            for k in range(top):
                col = width - edge + k
                value = info[:, col + top : col + top + 1] + info[:, col + 2 * top : col + 2 * top + 1]
                factor += jnp.where(info[:, col : col + 1] == expert, value, 0.0)
            factors.append(factor)
        x = jnp.concatenate([gathered[chunk(step), :width] for step in steps], axis=0)
        pieces = []
        for low_col, high_col in column_cuts(hidden_count, 256):
            g = lax.dot_general(x, vm_gate[low_col:high_col, :], NT, preferred_element_type=jnp.float32)
            u = lax.dot_general(x, vm_up[low_col:high_col, :], NT, preferred_element_type=jnp.float32)
            pieces.append((jax.nn.silu(g) * u).astype(jnp.bfloat16))
        hidden = jnp.concatenate(pieces, axis=1)
        if steps[0] == own:
            weights[2].wait()
        for low_col, high_col in column_cuts(width, 512):
            y = jnp.dot(hidden, vm_down[:, low_col:high_col], preferred_element_type=jnp.float32)
            for i, step in enumerate(steps):
                part = y[i * chunk_rows : (i + 1) * chunk_rows] * factors[i]
                partial[chunk(step), low_col:high_col] = part.astype(jnp.bfloat16)

    def pair(s, c):
        return pl.ds(pl.multiple_of((s * 2 + c) * fast * rows, rows), fast * rows)

    def tile(index):
        return pl.ds(pl.multiple_of(index * rows, rows), rows)

    def core_copy(step):
        s = source(step)
        return send(
            partial.at[pair(s, 1 - core)], from_core.at[pl.ds(step * fast * rows, fast * rows)],
            pass_send.at[step], pass_recv.at[step], name(at_slow, at_fast, 1 - core),
        )

    def both_cores(step, f):
        s = source(step)
        mine_part = partial[block(s, f, core), :].astype(jnp.float32)
        return mine_part + from_core[tile(step * fast + f), :].astype(jnp.float32)

    def fast_copy(step, off):
        place = pl.ds((step * (fast - 1) + off - 1) * rows, rows)
        return send(
            to_fast.at[place], from_fast.at[place],
            give_send.at[step, off], give_recv.at[step, off], name(at_slow, fast_at(off), core),
        )

    def slow_copy(step):
        place = pl.ds(step * rows, rows)
        return send(
            to_slow.at[place], from_slow.at[place],
            slow_send.at[step], slow_recv.at[step], name(source(step), at_fast, core),
        )

    def give_fast(step):
        core_copy(step).wait_recv()
        for off in range(1, fast):
            place = (step * (fast - 1) + off - 1) * rows
            to_fast[place : place + rows, :] = both_cores(step, fast_at(off)).astype(jnp.bfloat16)
            launch(fast_copy(step, off))

    first, second = order[: slow // 2], order[slow // 2 :]
    for step in first:
        take_slow(step)
    for step in first:
        take_fast(step)
    for step in second[:-1]:
        take_slow(step)
    for step in first:
        take_core(step)
    weights[0].wait()
    weights[1].wait()
    half_expert(first)
    for step in first[1:] + first[:1]:
        launch(core_copy(step))
    take_slow(second[-1])
    for step in second:
        take_fast(step)
    for step in first[1:] + first[:1]:
        give_fast(step)
    for step in second:
        take_core(step)
    half_expert(second)
    for step in second:
        launch(core_copy(step))
    for step in second:
        give_fast(step)
    for step in range(slow):
        total = both_cores(step, at_fast)
        for off in range(1, fast):
            fast_copy(step, off).wait_recv()
            place = (step * (fast - 1) + off - 1) * rows
            total += from_fast[place : place + rows, :].astype(jnp.float32)
        if offsets[step]:
            to_slow[step * rows : (step + 1) * rows, :] = total.astype(jnp.bfloat16)
            launch(slow_copy(step))
    for step in range(slow - 1):
        slow_copy(step).wait_recv()
        total += from_slow[step * rows : (step + 1) * rows, :].astype(jnp.float32)
    out[...] = total.astype(out.dtype)
    for copy in started:
        copy.wait_send()


def dense_local(slow, fast, tokens, routes, gate_fixed, gate_weight, up_weight, down_weight):
    rows, width = tokens.shape
    top = routes.shape[1]
    gate_weight = jnp.swapaxes(gate_weight, 1, 2)
    up_weight = jnp.swapaxes(up_weight, 1, 2)
    padded = -(-(width + 3 * top) // 128) * 128
    every = slow * fast * 2 * rows
    dma = pltpu.SemaphoreType.DMA
    half = slow * fast * rows
    vmem = pl.BlockSpec(memory_space=pltpu.VMEM)
    anywhere = pl.BlockSpec(memory_space=pl.ANY)
    return pl.pallas_call(
        functools.partial(dense_kernel, slow, fast),
        out_shape=jax.ShapeDtypeStruct((rows, width), jnp.bfloat16),
        in_specs=[vmem, vmem, vmem, anywhere, anywhere, anywhere],
        out_specs=vmem,
        scratch_shapes=[
            pltpu.VMEM((every, padded), jnp.bfloat16),
            pltpu.VMEM(gate_weight.shape[1:], jnp.bfloat16),
            pltpu.VMEM(up_weight.shape[1:], jnp.bfloat16),
            pltpu.VMEM(down_weight.shape[1:], jnp.bfloat16),
            pltpu.VMEM((every, width), jnp.bfloat16),
            pltpu.VMEM((half, width), jnp.bfloat16),
            pltpu.VMEM((slow * (fast - 1) * rows, width), jnp.bfloat16),
            pltpu.VMEM((slow * (fast - 1) * rows, width), jnp.bfloat16),
            pltpu.VMEM(((slow - 1) * rows, width), jnp.bfloat16),
            pltpu.VMEM(((slow - 1) * rows, width), jnp.bfloat16),
            dma((3,)),
            dma((slow,)), dma((slow,)),
            dma((slow * fast,)), dma((slow * fast,)),
            dma((slow, fast)), dma((slow, fast)),
            dma((slow,)), dma((slow,)),
            dma((slow,)), dma((slow,)),
            dma((slow, fast)), dma((slow, fast)),
        ],
        compiler_params=pltpu.CompilerParams(
            collective_id=0, has_side_effects=True, vmem_limit_bytes=60 * 2**20
        ),
    )(tokens, routes.T, gate_fixed.T, gate_weight, up_weight, down_weight)


def solution(mesh):
    placed = (
        P(("groups", "ep"), None),
        P(("groups", "ep"), None),
        P(("groups", "ep"), None),
        P("ep", None, None),
        P("ep", None, None),
        P("ep", None, None),
    )
    chips = mesh.shape["ep"] // 2

    def body(*args):
        top = args[1].shape[1]
        if chips <= 4 * top and chips % 4 == 0:
            return dense_local(4, chips // 4, *args)
        return local(*args)

    return jax.shard_map(
        body, mesh=mesh, in_specs=placed, out_specs=P(("groups", "ep"), None), check_vma=False
    )
```

```python
import functools

import jax
import jax.numpy as jnp
from jax import lax
from jax.experimental import pallas as pl
from jax.experimental.pallas import tpu as pltpu
from jax.sharding import PartitionSpec as P


def swapped(value, axis, bit):
    mask = 2**bit
    pairs = [(source, source ^ mask) for source in range(lax.axis_size(axis))]
    return lax.ppermute(value, axis, pairs)


def expert_half(expert_rows, w_gate, w_up, w_down):
    gate_part = jnp.dot(expert_rows, w_gate, preferred_element_type=jnp.float32)
    up_part = jnp.dot(expert_rows, w_up, preferred_element_type=jnp.float32)
    hidden = (jax.nn.silu(gate_part) * up_part).astype(jnp.bfloat16)
    return jnp.dot(hidden, w_down, preferred_element_type=jnp.float32).astype(jnp.bfloat16)


def local(tokens, routes, gate_fixed, gate_weight, up_weight, down_weight):
    devices_ep = lax.axis_size("ep")
    experts = devices_ep // 2
    tok_count = tokens.shape[0]
    top_count = routes.shape[1]
    width = tokens.shape[1]
    capacity = 2 * tok_count * top_count // experts
    onehot = (routes[:, :, None] == jnp.arange(experts, dtype=jnp.int32)).astype(jnp.int32)
    flat_hot = onehot.reshape(tok_count * top_count, experts)
    before = jnp.cumsum(flat_hot, axis=0) - flat_hot
    position = jnp.sum(before * flat_hot, axis=1).reshape(tok_count, top_count)
    slot_index = routes * capacity + position
    select = (slot_index[:, :, None] == jnp.arange(experts * capacity, dtype=jnp.int32)).astype(
        jnp.int32
    )
    select = jnp.sum(select, axis=1).astype(jnp.bfloat16)
    packed = jnp.einsum("ts,td->sd", select, tokens, preferred_element_type=jnp.float32).astype(
        jnp.bfloat16
    )
    packed = packed.reshape(experts, 1, capacity, width)
    outgoing = jnp.broadcast_to(packed, (experts, 2, capacity, width)).reshape(
        devices_ep, capacity, width
    )
    received = lax.all_to_all(outgoing, "ep", split_axis=0, concat_axis=0, tiled=True)
    result = expert_half(received.reshape(-1, width), gate_weight[0], up_weight[0], down_weight[0])
    partial_value = result.reshape(received.shape[0], received.shape[1], width)
    parity = lax.axis_index("ep") % 2
    halves = partial_value.reshape(devices_ep, capacity, 2, width // 2)
    kept_half = lax.dynamic_index_in_dim(halves, parity, 2, keepdims=False)
    given_half = lax.dynamic_index_in_dim(halves, 1 - parity, 2, keepdims=False)
    partner = swapped(given_half, "ep", 0)
    reduced = (kept_half.astype(jnp.float32) + partner.astype(jnp.float32)).astype(jnp.bfloat16)
    returned = lax.all_to_all(reduced, "ep", split_axis=0, concat_axis=0, tiled=True)
    ordered = returned.reshape(experts, 2, capacity, width // 2).transpose(0, 2, 1, 3)
    expert_out = ordered.reshape(experts * capacity, width)
    picked = jnp.take(expert_out, slot_index.reshape(-1), axis=0).reshape(
        tok_count, top_count, width
    )
    weights = gate_fixed.astype(jnp.float32) / 65536.0
    mixed = jnp.sum(weights[:, :, None] * picked.astype(jnp.float32), axis=1)
    return mixed.astype(jnp.bfloat16)


NT = (((1,), (1,)), ((), ()))


def column_cuts(width, step):
    return [(low, min(low + step, width)) for low in range(0, width, step)]


def dense_kernel(
    slow, fast, tokens, routes, gates, w_gate, w_up, w_down, out,
    gathered, vm_gate, vm_up, vm_down, partial, from_core, to_fast, from_fast, to_slow, from_slow,
    w_sem, ag_send, ag_recv, core_send, core_recv, fast_send, fast_recv, slow_send, slow_recv,
    pass_send, pass_recv, give_send, give_recv,
):
    rows, width = tokens.shape
    top = routes.shape[0]
    padded = gathered.shape[1]
    hidden_count = vm_gate.shape[0]
    device = lax.axis_index("ep")
    core = lax.rem(device, 2)
    chip = device // 2
    at_slow = chip // fast
    at_fast = lax.rem(chip, fast)

    weights = [
        pltpu.make_async_copy(source.at[0], target, w_sem.at[i])
        for i, (source, target) in enumerate(((w_gate, vm_gate), (w_up, vm_up), (w_down, vm_down)))
    ]
    for copy in weights:
        copy.start()

    def name(s, f, c):
        return {"ep": (s * fast + f) * 2 + c}

    def slow_at(off):
        return lax.rem(at_slow + off, slow)

    def fast_at(off):
        return lax.rem(at_fast + off, fast)

    def block(s, f, c):
        start = ((s * 2 + c) * fast + f) * rows
        return pl.ds(pl.multiple_of(start, rows), rows)

    def send(source, target, send_sem, recv_sem, device_id):
        return pltpu.make_async_remote_copy(
            src_ref=source, dst_ref=target, send_sem=send_sem, recv_sem=recv_sem,
            device_id=device_id, device_id_type=pl.DeviceIdType.MESH,
        )

    peers = [name(slow_at(off), at_fast, core) for off in range(1, slow)]
    peers += [name(at_slow, fast_at(off), core) for off in range(1, fast)]
    peers += [name(at_slow, at_fast, 1 - core)]
    barrier = pltpu.get_barrier_semaphore()
    for peer in peers:
        pl.semaphore_signal(barrier, inc=1, device_id=peer, device_id_type=pl.DeviceIdType.MESH)

    mine = block(at_slow, at_fast, core)
    edge = width // 128 * 128
    lanes = lax.broadcasted_iota(jnp.int32, (rows, padded - edge), 1) + edge
    gathered[mine, edge:] = jnp.zeros((rows, padded - edge), jnp.bfloat16)
    gathered[mine, :width] = tokens[...]
    scale = jnp.transpose(gates[...].astype(jnp.float32)) / 65536.0
    high = scale.astype(jnp.bfloat16).astype(jnp.float32)
    low = scale - high
    ids = jnp.transpose(routes[...].astype(jnp.float32))
    tail = gathered[mine, edge:].astype(jnp.float32)
    for k in range(top):
        tail = jnp.where(lanes == width + k, ids[:, k : k + 1], tail)
        tail = jnp.where(lanes == width + top + k, high[:, k : k + 1], tail)
        tail = jnp.where(lanes == width + 2 * top + k, low[:, k : k + 1], tail)
    gathered[mine, edge:] = tail.astype(jnp.bfloat16)

    pl.semaphore_wait(barrier, len(peers))

    started = []

    def launch(copy):
        copy.start()
        started.append(copy)

    def to_partner(s, f, slot):
        where = gathered.at[block(s, f, core)]
        launch(send(where, where, core_send.at[slot], core_recv.at[slot], name(at_slow, at_fast, 1 - core)))

    def along_fast(s, step):
        where = gathered.at[block(s, at_fast, core)]
        for off in range(1, fast):
            launch(send(where, where, fast_send.at[step, off], fast_recv.at[step, off], name(at_slow, fast_at(off), core)))

    here = gathered.at[mine]
    along_fast(at_slow, slow - 1)
    outward, across = at_slow + 1 - 2 * lax.rem(at_slow, 2), slow - 1 - at_slow
    inner = (at_slow % 3) != 0

    def to_slow_chip(s, place, sem, slot):
        where = gathered.at[block(s, at_fast, core)]
        return send(where, where, ag_send.at[sem], ag_recv.at[slot], name(place, at_fast, core))

    to_slow_chip(at_slow, outward, 0, 0).start()

    @pl.when(inner)
    def _():
        to_slow_chip(at_slow, across, 1, 1).start()

    to_partner(at_slow, at_fast, (slow - 1) * fast)

    own = slow - 1
    order = [own] + list(range(own))
    chunk_rows = 2 * fast * rows

    def source(step):
        return [outward, 2 - at_slow // 2, 3 - 3 * (at_slow // 2), at_slow][step]

    def take_slow(step):
        if step == own:
            return
        s = source(step)
        got = gathered.at[block(s, at_fast, core)]
        send(got, got, ag_send.at[step], ag_recv.at[step], name(outward, at_fast, core)).wait_recv()

        @pl.when(inner)
        def _():
            if step == 0:
                to_slow_chip(s, across, 2, 2).start()
            else:
                to_slow_chip(s, outward, 2 + step, step).start()

        along_fast(s, step)
        to_partner(s, at_fast, step * fast)

    def take_fast(step):
        for off in range(1, fast):
            f = fast_at(fast - off)
            got = gathered.at[block(source(step), f, core)]
            send(got, got, fast_send.at[step, off], fast_recv.at[step, off], name(at_slow, f, core)).wait_recv()
            to_partner(source(step), f, step * fast + off)

    def take_core(step):
        for off in range(fast):
            slot = step * fast + off
            got = gathered.at[block(source(step), fast_at(fast - off), 1 - core)]
            send(got, got, core_send.at[slot], core_recv.at[slot], name(at_slow, at_fast, 1 - core)).wait_recv()

    def chunk(step):
        return pl.ds(pl.multiple_of(source(step) * chunk_rows, chunk_rows), chunk_rows)

    def half_expert(steps):
        expert = chip.astype(jnp.float32)
        factors = []
        for step in steps:
            info = gathered[chunk(step), edge:].astype(jnp.float32)
            factor = jnp.zeros((chunk_rows, 1), jnp.float32)
            for k in range(top):
                col = width - edge + k
                value = info[:, col + top : col + top + 1] + info[:, col + 2 * top : col + 2 * top + 1]
                factor += jnp.where(info[:, col : col + 1] == expert, value, 0.0)
            factors.append(factor)
        x = jnp.concatenate([gathered[chunk(step), :width] for step in steps], axis=0)
        pieces = []
        for low_col, high_col in column_cuts(hidden_count, 256):
            g = lax.dot_general(x, vm_gate[low_col:high_col, :], NT, preferred_element_type=jnp.float32)
            u = lax.dot_general(x, vm_up[low_col:high_col, :], NT, preferred_element_type=jnp.float32)
            pieces.append((jax.nn.silu(g) * u).astype(jnp.bfloat16))
        hidden = jnp.concatenate(pieces, axis=1)
        if steps[0] == own:
            weights[2].wait()
        for low_col, high_col in column_cuts(width, 512):
            y = jnp.dot(hidden, vm_down[:, low_col:high_col], preferred_element_type=jnp.float32)
            for i, step in enumerate(steps):
                part = y[i * chunk_rows : (i + 1) * chunk_rows] * factors[i]
                partial[chunk(step), low_col:high_col] = part.astype(jnp.bfloat16)

    def pair(s, c):
        return pl.ds(pl.multiple_of((s * 2 + c) * fast * rows, rows), fast * rows)

    def tile(index):
        return pl.ds(pl.multiple_of(index * rows, rows), rows)

    def core_copy(step):
        s = source(step)
        return send(
            partial.at[pair(s, 1 - core)], from_core.at[pl.ds(step * fast * rows, fast * rows)],
            pass_send.at[step], pass_recv.at[step], name(at_slow, at_fast, 1 - core),
        )

    def both_cores(step, f):
        s = source(step)
        mine_part = partial[block(s, f, core), :].astype(jnp.float32)
        return mine_part + from_core[tile(step * fast + f), :].astype(jnp.float32)

    def fast_copy(step, off):
        place = pl.ds((step * (fast - 1) + off - 1) * rows, rows)
        return send(
            to_fast.at[place], from_fast.at[place],
            give_send.at[step, off], give_recv.at[step, off], name(at_slow, fast_at(off), core),
        )

    def slow_copy(step):
        return send(
            to_slow.at[pl.ds(step * rows, rows)], from_slow.at[tile(at_slow)],
            slow_send.at[step], slow_recv.at[at_slow], name(source(step), at_fast, core),
        )

    def give_fast(step):
        core_copy(step).wait_recv()
        for off in range(1, fast):
            place = (step * (fast - 1) + off - 1) * rows
            to_fast[place : place + rows, :] = both_cores(step, fast_at(off)).astype(jnp.bfloat16)
            launch(fast_copy(step, off))

    first, second = order[: slow // 2], order[slow // 2 :]
    take_slow(0)
    take_slow(1)
    take_fast(own)
    take_fast(0)
    take_slow(2)
    take_fast(1)
    for step in first:
        take_core(step)
    weights[0].wait()
    weights[1].wait()
    half_expert(first)
    for step in first[1:] + first[:1]:
        launch(core_copy(step))
    take_fast(2)
    for step in first[1:] + first[:1]:
        give_fast(step)
    for step in second:
        take_core(step)
    half_expert(second)
    for step in second:
        launch(core_copy(step))
    for step in second:
        give_fast(step)
    for step in range(slow):
        total = both_cores(step, at_fast)
        for off in range(1, fast):
            fast_copy(step, off).wait_recv()
            place = (step * (fast - 1) + off - 1) * rows
            total += from_fast[place : place + rows, :].astype(jnp.float32)
        if step != own:
            to_slow[step * rows : (step + 1) * rows, :] = total.astype(jnp.bfloat16)
            launch(slow_copy(step))
    for off in range(1, slow):
        s = slow_at(off)
        got = from_slow.at[tile(s)]
        send(got, got, slow_send.at[0], slow_recv.at[s], name(s, at_fast, core)).wait_recv()
        total += from_slow[tile(s), :].astype(jnp.float32)
    out[...] = total.astype(out.dtype)
    for copy in started:
        copy.wait_send()
    to_slow_chip(at_slow, outward, 0, 0).wait_send()

    @pl.when(inner)
    def _():
        for sem in range(1, 5):
            to_slow_chip(at_slow, outward, sem, 0).wait_send()


def dense_local(slow, fast, tokens, routes, gate_fixed, gate_weight, up_weight, down_weight):
    rows, width = tokens.shape
    top = routes.shape[1]
    gate_weight = jnp.swapaxes(gate_weight, 1, 2)
    up_weight = jnp.swapaxes(up_weight, 1, 2)
    padded = -(-(width + 3 * top) // 128) * 128
    every = slow * fast * 2 * rows
    dma = pltpu.SemaphoreType.DMA
    half = slow * fast * rows
    vmem = pl.BlockSpec(memory_space=pltpu.VMEM)
    anywhere = pl.BlockSpec(memory_space=pl.ANY)
    return pl.pallas_call(
        functools.partial(dense_kernel, slow, fast),
        out_shape=jax.ShapeDtypeStruct((rows, width), jnp.bfloat16),
        in_specs=[vmem, vmem, vmem, anywhere, anywhere, anywhere],
        out_specs=vmem,
        scratch_shapes=[
            pltpu.VMEM((every, padded), jnp.bfloat16),
            pltpu.VMEM(gate_weight.shape[1:], jnp.bfloat16),
            pltpu.VMEM(up_weight.shape[1:], jnp.bfloat16),
            pltpu.VMEM(down_weight.shape[1:], jnp.bfloat16),
            pltpu.VMEM((every, width), jnp.bfloat16),
            pltpu.VMEM((half, width), jnp.bfloat16),
            pltpu.VMEM((slow * (fast - 1) * rows, width), jnp.bfloat16),
            pltpu.VMEM((slow * (fast - 1) * rows, width), jnp.bfloat16),
            pltpu.VMEM(((slow - 1) * rows, width), jnp.bfloat16),
            pltpu.VMEM((slow * rows, width), jnp.bfloat16),
            dma((3,)),
            dma((5,)), dma((3,)),
            dma((slow * fast,)), dma((slow * fast,)),
            dma((slow, fast)), dma((slow, fast)),
            dma((slow,)), dma((slow,)),
            dma((slow,)), dma((slow,)),
            dma((slow, fast)), dma((slow, fast)),
        ],
        compiler_params=pltpu.CompilerParams(
            collective_id=0, has_side_effects=True, vmem_limit_bytes=60 * 2**20
        ),
    )(tokens, routes.T, gate_fixed.T, gate_weight, up_weight, down_weight)


def solution(mesh):
    placed = (
        P(("groups", "ep"), None),
        P(("groups", "ep"), None),
        P(("groups", "ep"), None),
        P("ep", None, None),
        P("ep", None, None),
        P("ep", None, None),
    )
    chips = mesh.shape["ep"] // 2

    def body(*args):
        top = args[1].shape[1]
        if chips <= 4 * top and chips % 4 == 0:
            return dense_local(4, chips // 4, *args)
        return local(*args)

    return jax.shard_map(
        body, mesh=mesh, in_specs=placed, out_specs=P(("groups", "ep"), None), check_vma=False
    )
```

```python
import functools

import jax
import jax.numpy as jnp
from jax import lax
from jax.experimental import pallas as pl
from jax.experimental.pallas import tpu as pltpu
from jax.sharding import PartitionSpec as P


def swapped(value, axis, bit):
    mask = 2**bit
    pairs = [(source, source ^ mask) for source in range(lax.axis_size(axis))]
    return lax.ppermute(value, axis, pairs)


def expert_half(expert_rows, w_gate, w_up, w_down):
    gate_part = jnp.dot(expert_rows, w_gate, preferred_element_type=jnp.float32)
    up_part = jnp.dot(expert_rows, w_up, preferred_element_type=jnp.float32)
    hidden = (jax.nn.silu(gate_part) * up_part).astype(jnp.bfloat16)
    return jnp.dot(hidden, w_down, preferred_element_type=jnp.float32).astype(jnp.bfloat16)


def local(tokens, routes, gate_fixed, gate_weight, up_weight, down_weight):
    devices_ep = lax.axis_size("ep")
    experts = devices_ep // 2
    tok_count = tokens.shape[0]
    top_count = routes.shape[1]
    width = tokens.shape[1]
    capacity = 2 * tok_count * top_count // experts
    onehot = (routes[:, :, None] == jnp.arange(experts, dtype=jnp.int32)).astype(jnp.int32)
    flat_hot = onehot.reshape(tok_count * top_count, experts)
    before = jnp.cumsum(flat_hot, axis=0) - flat_hot
    position = jnp.sum(before * flat_hot, axis=1).reshape(tok_count, top_count)
    slot_index = routes * capacity + position
    select = (slot_index[:, :, None] == jnp.arange(experts * capacity, dtype=jnp.int32)).astype(
        jnp.int32
    )
    select = jnp.sum(select, axis=1).astype(jnp.bfloat16)
    packed = jnp.einsum("ts,td->sd", select, tokens, preferred_element_type=jnp.float32).astype(
        jnp.bfloat16
    )
    packed = packed.reshape(experts, 1, capacity, width)
    outgoing = jnp.broadcast_to(packed, (experts, 2, capacity, width)).reshape(
        devices_ep, capacity, width
    )
    received = lax.all_to_all(outgoing, "ep", split_axis=0, concat_axis=0, tiled=True)
    result = expert_half(received.reshape(-1, width), gate_weight[0], up_weight[0], down_weight[0])
    partial_value = result.reshape(received.shape[0], received.shape[1], width)
    parity = lax.axis_index("ep") % 2
    halves = partial_value.reshape(devices_ep, capacity, 2, width // 2)
    kept_half = lax.dynamic_index_in_dim(halves, parity, 2, keepdims=False)
    given_half = lax.dynamic_index_in_dim(halves, 1 - parity, 2, keepdims=False)
    partner = swapped(given_half, "ep", 0)
    reduced = (kept_half.astype(jnp.float32) + partner.astype(jnp.float32)).astype(jnp.bfloat16)
    returned = lax.all_to_all(reduced, "ep", split_axis=0, concat_axis=0, tiled=True)
    ordered = returned.reshape(experts, 2, capacity, width // 2).transpose(0, 2, 1, 3)
    expert_out = ordered.reshape(experts * capacity, width)
    picked = jnp.take(expert_out, slot_index.reshape(-1), axis=0).reshape(
        tok_count, top_count, width
    )
    weights = gate_fixed.astype(jnp.float32) / 65536.0
    mixed = jnp.sum(weights[:, :, None] * picked.astype(jnp.float32), axis=1)
    return mixed.astype(jnp.bfloat16)


NT = (((1,), (1,)), ((), ()))


def column_cuts(width, step):
    return [(low, min(low + step, width)) for low in range(0, width, step)]


def dense_kernel(
    slow, fast, tokens, routes, gates, w_gate, w_up, w_down, out,
    gathered, vm_gate, vm_up, vm_down, partial, from_core, to_fast, from_fast, to_slow, from_slow,
    w_sem, ag_send, ag_recv, core_send, core_recv, fast_send, fast_recv, slow_send, slow_recv,
    pass_send, pass_recv, give_send, give_recv,
):
    rows, width = tokens.shape
    top = routes.shape[0]
    padded = gathered.shape[1]
    hidden_count = vm_gate.shape[0]
    device = lax.axis_index("ep")
    core = lax.rem(device, 2)
    chip = device // 2
    at_slow = chip // fast
    at_fast = lax.rem(chip, fast)

    weights = [
        pltpu.make_async_copy(source.at[0], target, w_sem.at[i])
        for i, (source, target) in enumerate(((w_gate, vm_gate), (w_up, vm_up), (w_down, vm_down)))
    ]
    for copy in weights:
        copy.start()

    def name(s, f, c):
        return {"ep": (s * fast + f) * 2 + c}

    def slow_at(off):
        return lax.rem(at_slow + off, slow)

    def fast_at(off):
        return lax.rem(at_fast + off, fast)

    def block(s, f, c):
        start = ((s * 2 + c) * fast + f) * rows
        return pl.ds(pl.multiple_of(start, rows), rows)

    def send(source, target, send_sem, recv_sem, device_id):
        return pltpu.make_async_remote_copy(
            src_ref=source, dst_ref=target, send_sem=send_sem, recv_sem=recv_sem,
            device_id=device_id, device_id_type=pl.DeviceIdType.MESH,
        )

    peers = [name(slow_at(off), at_fast, core) for off in range(1, slow)]
    peers += [name(at_slow, fast_at(off), core) for off in range(1, fast)]
    peers += [name(at_slow, at_fast, 1 - core)]
    barrier = pltpu.get_barrier_semaphore()
    for peer in peers:
        pl.semaphore_signal(barrier, inc=1, device_id=peer, device_id_type=pl.DeviceIdType.MESH)

    mine = block(at_slow, at_fast, core)
    edge = width // 128 * 128
    lanes = lax.broadcasted_iota(jnp.int32, (rows, padded - edge), 1) + edge
    gathered[mine, edge:] = jnp.zeros((rows, padded - edge), jnp.bfloat16)
    gathered[mine, :width] = tokens[...]
    scale = jnp.transpose(gates[...].astype(jnp.float32)) / 65536.0
    high = scale.astype(jnp.bfloat16).astype(jnp.float32)
    low = scale - high
    ids = jnp.transpose(routes[...].astype(jnp.float32))
    tail = gathered[mine, edge:].astype(jnp.float32)
    for k in range(top):
        tail = jnp.where(lanes == width + k, ids[:, k : k + 1], tail)
        tail = jnp.where(lanes == width + top + k, high[:, k : k + 1], tail)
        tail = jnp.where(lanes == width + 2 * top + k, low[:, k : k + 1], tail)
    gathered[mine, edge:] = tail.astype(jnp.bfloat16)

    pl.semaphore_wait(barrier, len(peers))

    started = []

    def launch(copy):
        copy.start()
        started.append(copy)

    def to_partner(s, f, slot):
        where = gathered.at[block(s, f, core)]
        launch(send(where, where, core_send.at[slot], core_recv.at[slot], name(at_slow, at_fast, 1 - core)))

    def along_fast(s, step):
        where = gathered.at[block(s, at_fast, core)]
        for off in range(1, fast):
            launch(send(where, where, fast_send.at[step, off], fast_recv.at[step, off], name(at_slow, fast_at(off), core)))

    here = gathered.at[mine]
    along_fast(at_slow, slow - 1)
    outward, across = at_slow + 1 - 2 * lax.rem(at_slow, 2), slow - 1 - at_slow
    inner = (at_slow % 3) != 0

    def to_slow_chip(s, place, sem, slot):
        where = gathered.at[block(s, at_fast, core)]
        return send(where, where, ag_send.at[sem], ag_recv.at[slot], name(place, at_fast, core))

    to_slow_chip(at_slow, outward, 0, 0).start()

    @pl.when(inner)
    def _():
        to_slow_chip(at_slow, across, 1, 1).start()

    to_partner(at_slow, at_fast, (slow - 1) * fast)

    own = slow - 1
    order = [own] + list(range(own))
    chunk_rows = 2 * fast * rows

    def source(step):
        return [outward, 2 - at_slow // 2, 3 - 3 * (at_slow // 2), at_slow][step]

    def take_slow(step):
        if step == own:
            return
        s = source(step)
        got = gathered.at[block(s, at_fast, core)]
        send(got, got, ag_send.at[step], ag_recv.at[step], name(outward, at_fast, core)).wait_recv()

        @pl.when(inner)
        def _():
            if step == 0:
                to_slow_chip(s, across, 2, 2).start()
            else:
                to_slow_chip(s, outward, 2 + step, step).start()

        along_fast(s, step)
        to_partner(s, at_fast, step * fast)

    def take_fast(step):
        for off in range(1, fast):
            f = fast_at(fast - off)
            got = gathered.at[block(source(step), f, core)]
            send(got, got, fast_send.at[step, off], fast_recv.at[step, off], name(at_slow, f, core)).wait_recv()
            to_partner(source(step), f, step * fast + off)

    def take_core(step):
        for off in range(fast):
            slot = step * fast + off
            got = gathered.at[block(source(step), fast_at(fast - off), 1 - core)]
            send(got, got, core_send.at[slot], core_recv.at[slot], name(at_slow, at_fast, 1 - core)).wait_recv()

    def chunk(step):
        return pl.ds(pl.multiple_of(source(step) * chunk_rows, chunk_rows), chunk_rows)

    def half_expert(steps):
        expert = chip.astype(jnp.float32)
        factors = []
        for step in steps:
            info = gathered[chunk(step), edge:].astype(jnp.float32)
            factor = jnp.zeros((chunk_rows, 1), jnp.float32)
            for k in range(top):
                col = width - edge + k
                value = info[:, col + top : col + top + 1] + info[:, col + 2 * top : col + 2 * top + 1]
                factor += jnp.where(info[:, col : col + 1] == expert, value, 0.0)
            factors.append(factor)
        x = jnp.concatenate([gathered[chunk(step), :width] for step in steps], axis=0)
        pieces = []
        for low_col, high_col in column_cuts(hidden_count, 256):
            g = lax.dot_general(x, vm_gate[low_col:high_col, :], NT, preferred_element_type=jnp.float32)
            u = lax.dot_general(x, vm_up[low_col:high_col, :], NT, preferred_element_type=jnp.float32)
            pieces.append((jax.nn.silu(g) * u).astype(jnp.bfloat16))
        hidden = jnp.concatenate(pieces, axis=1)
        if steps[0] == own:
            weights[2].wait()
        for low_col, high_col in column_cuts(width, 512):
            y = jnp.dot(hidden, vm_down[:, low_col:high_col], preferred_element_type=jnp.float32)
            for i, step in enumerate(steps):
                part = y[i * chunk_rows : (i + 1) * chunk_rows] * factors[i]
                partial[chunk(step), low_col:high_col] = part.astype(jnp.bfloat16)

    def pair(s, c):
        return pl.ds(pl.multiple_of((s * 2 + c) * fast * rows, rows), fast * rows)

    def tile(index):
        return pl.ds(pl.multiple_of(index * rows, rows), rows)

    def core_copy(step):
        s = source(step)
        return send(
            partial.at[pair(s, 1 - core)], from_core.at[pl.ds(step * fast * rows, fast * rows)],
            pass_send.at[step], pass_recv.at[step], name(at_slow, at_fast, 1 - core),
        )

    def both_cores(step, f):
        s = source(step)
        mine_part = partial[block(s, f, core), :].astype(jnp.float32)
        return mine_part + from_core[tile(step * fast + f), :].astype(jnp.float32)

    def fast_copy(step, off):
        place = pl.ds((step * (fast - 1) + off - 1) * rows, rows)
        return send(
            to_fast.at[place], from_fast.at[place],
            give_send.at[step, off], give_recv.at[step, off], name(at_slow, fast_at(off), core),
        )

    def slow_copy(step):
        return send(
            to_slow.at[pl.ds(step * rows, rows)], from_slow.at[tile(at_slow)],
            slow_send.at[step], slow_recv.at[at_slow], name(source(step), at_fast, core),
        )

    def give_fast(step):
        core_copy(step).wait_recv()
        for off in range(1, fast):
            place = (step * (fast - 1) + off - 1) * rows
            to_fast[place : place + rows, :] = both_cores(step, fast_at(off)).astype(jnp.bfloat16)
            launch(fast_copy(step, off))

    first, second = order[: slow // 2], order[slow // 2 :]
    take_slow(0)
    take_slow(1)
    take_fast(own)
    take_fast(0)
    take_slow(2)
    take_fast(1)
    for step in first:
        take_core(step)
    weights[0].wait()
    weights[1].wait()
    half_expert(first)
    for step in first[1:] + first[:1]:
        launch(core_copy(step))
    take_fast(2)
    for step in first[1:] + first[:1]:
        give_fast(step)
    for step in second:
        take_core(step)
    half_expert(second)
    for step in second[::-1]:
        launch(core_copy(step))

    def finish(step):
        total = both_cores(step, at_fast)
        for off in range(1, fast):
            fast_copy(step, off).wait_recv()
            place = (step * (fast - 1) + off - 1) * rows
            total += from_fast[place : place + rows, :].astype(jnp.float32)
        if step == own:
            return total
        to_slow[step * rows : (step + 1) * rows, :] = total.astype(jnp.bfloat16)
        launch(slow_copy(step))

    finish(0)
    for step in second[::-1]:
        give_fast(step)
    for step in second[::-1]:
        finish(step)
    total = finish(own)
    for off in range(1, slow):
        s = slow_at(off)
        got = from_slow.at[tile(s)]
        send(got, got, slow_send.at[0], slow_recv.at[s], name(s, at_fast, core)).wait_recv()
        total += from_slow[tile(s), :].astype(jnp.float32)
    out[...] = total.astype(out.dtype)
    for copy in started:
        copy.wait_send()
    to_slow_chip(at_slow, outward, 0, 0).wait_send()

    @pl.when(inner)
    def _():
        for sem in range(1, 5):
            to_slow_chip(at_slow, outward, sem, 0).wait_send()


def dense_local(slow, fast, tokens, routes, gate_fixed, gate_weight, up_weight, down_weight):
    rows, width = tokens.shape
    top = routes.shape[1]
    gate_weight = jnp.swapaxes(gate_weight, 1, 2)
    up_weight = jnp.swapaxes(up_weight, 1, 2)
    padded = -(-(width + 3 * top) // 128) * 128
    every = slow * fast * 2 * rows
    dma = pltpu.SemaphoreType.DMA
    half = slow * fast * rows
    vmem = pl.BlockSpec(memory_space=pltpu.VMEM)
    anywhere = pl.BlockSpec(memory_space=pl.ANY)
    return pl.pallas_call(
        functools.partial(dense_kernel, slow, fast),
        out_shape=jax.ShapeDtypeStruct((rows, width), jnp.bfloat16),
        in_specs=[vmem, vmem, vmem, anywhere, anywhere, anywhere],
        out_specs=vmem,
        scratch_shapes=[
            pltpu.VMEM((every, padded), jnp.bfloat16),
            pltpu.VMEM(gate_weight.shape[1:], jnp.bfloat16),
            pltpu.VMEM(up_weight.shape[1:], jnp.bfloat16),
            pltpu.VMEM(down_weight.shape[1:], jnp.bfloat16),
            pltpu.VMEM((every, width), jnp.bfloat16),
            pltpu.VMEM((half, width), jnp.bfloat16),
            pltpu.VMEM((slow * (fast - 1) * rows, width), jnp.bfloat16),
            pltpu.VMEM((slow * (fast - 1) * rows, width), jnp.bfloat16),
            pltpu.VMEM(((slow - 1) * rows, width), jnp.bfloat16),
            pltpu.VMEM((slow * rows, width), jnp.bfloat16),
            dma((3,)),
            dma((5,)), dma((3,)),
            dma((slow * fast,)), dma((slow * fast,)),
            dma((slow, fast)), dma((slow, fast)),
            dma((slow,)), dma((slow,)),
            dma((slow,)), dma((slow,)),
            dma((slow, fast)), dma((slow, fast)),
        ],
        compiler_params=pltpu.CompilerParams(
            collective_id=0, has_side_effects=True, vmem_limit_bytes=60 * 2**20
        ),
    )(tokens, routes.T, gate_fixed.T, gate_weight, up_weight, down_weight)


def solution(mesh):
    placed = (
        P(("groups", "ep"), None),
        P(("groups", "ep"), None),
        P(("groups", "ep"), None),
        P("ep", None, None),
        P("ep", None, None),
        P("ep", None, None),
    )
    chips = mesh.shape["ep"] // 2

    def body(*args):
        top = args[1].shape[1]
        if chips <= 4 * top and chips % 4 == 0:
            return dense_local(4, chips // 4, *args)
        return local(*args)

    return jax.shard_map(
        body, mesh=mesh, in_specs=placed, out_specs=P(("groups", "ep"), None), check_vma=False
    )
```
